32 devices in a mesh: dp: 8 (over z, y), tensor: 4 (over x, core).
Axes of the slice: x: 2, y: 2, z: 4, core: 2. Of those that a mesh axis runs over, the one named last changes fastest.
Arguments:
- queries: bfloat16 [16, 512, 3072], P('dp', None, 'tensor'), may hold values from -110 to 110
- draft_key_value: bfloat16 [16, 2, 512, 512], P('dp', None, None, 'tensor'), may hold values from -4.5 to 4.5
- cache_kv: bfloat16 [16, 2, 1792, 512], P('dp', None, None, 'tensor'), may hold values from -6 to 6
- out_weight: bfloat16 [3072, 6144], P('tensor'), may hold values from -0.109375 to 0.109375
- tree_sizes: int32 [16], replicated, may hold values from 16 to 512
- parents: int32 [16, 512], replicated, may hold values from 0 to 511, as said below
- cache_lens: int32 [16], replicated, may hold values from 448 to 1792
- block_moves: int32 [8, 2], replicated, may hold values from 0 to 7, as said below
Outputs:
- own_out: bfloat16 [8192, 6144], P(('dp', 'tensor'))
- moved_out: bfloat16 [1024, 6144], P(('dp', 'tensor'))
The draws below stay inside these ranges and needn't reach their ends.
Inputs may be any that keep to these rules, and one draw needn't show every extreme that they name: parents[r, 0] = 0 and parents[r, i] < i for every i >= 1. `block_moves`: row d is (destination, slot). The destination is d itself (nothing moves, slot 0) or differs from d in exactly one bit. No device is the destination of two others, and a device that gives a block away takes none. A moved slot (r mod 2) * 4 + k names a block with k * 128 < tree_sizes[r] of one of d's requests r.
All inputs are finite; a program needn't handle non-finite values.
Results may differ from the reference program's by a relative error of at most 0.01.
Values may be sent and summed in bfloat16 or wider, within the bound.
A program may use at most 128 MiB of HBM per device.

```python
import jax
import jax.numpy as jnp
from jax import lax

D = 6144
QUERY_HEADS = 24
KEY_VALUE_HEADS = 4
HEAD_SIZE = 128
BLK = 128
MAXB = 4
REQ_DEV = 2
CACHE_SLOTS = 1792
TREE_ROWS = 512
REQUEST_COUNT = 16
N_DP = 8
N_TENSOR = 4


def stored_pairs(key):
    array_shape = (REQUEST_COUNT, 2, CACHE_SLOTS, KEY_VALUE_HEADS * HEAD_SIZE)
    values = jnp.clip(jax.random.normal(jax.random.fold_in(key, 105), array_shape, jnp.float32), -4.5, 4.5)
    return values


def draw_cache_kv(key, part):
    return stored_pairs(key).astype(jnp.bfloat16)


def draw_queries(key, part):
    array_shape = (REQUEST_COUNT, TREE_ROWS, QUERY_HEADS * HEAD_SIZE)
    values = jnp.clip(jax.random.normal(jax.random.fold_in(key, 103), array_shape, jnp.float32), -4.5, 4.5)
    return values.astype(jnp.bfloat16)


def tree_counts(key):
    spread = jax.random.randint(jax.random.fold_in(key, 101), (REQUEST_COUNT,), max(1, BLK // 8), TREE_ROWS + 1, jnp.int32)
    light = jax.random.randint(jax.random.fold_in(key, 108), (REQUEST_COUNT,), max(1, BLK // 8), BLK + 1, jnp.int32)
    owner = jnp.arange(REQUEST_COUNT, dtype=jnp.int32) // REQ_DEV
    within = owner % (N_DP // 2)
    counts = jnp.where(within == 0, light, spread)
    counts = jnp.where(within == 1, TREE_ROWS, counts)
    return counts.astype(jnp.int32)


def draw_tree_sizes(key, part):
    return tree_counts(key)


def draw_parents(key, part):
    position = jnp.arange(TREE_ROWS, dtype=jnp.int32)
    upper = jnp.maximum(position, 1)
    return jax.random.randint(jax.random.fold_in(key, 107), (REQUEST_COUNT, TREE_ROWS), 0, upper[None, :], jnp.int32)


def draw_block_moves(key, part):
    blocks = ((tree_counts(key) + BLK - 1) // BLK).reshape(N_DP, REQ_DEV)
    loads = jnp.sum(blocks, axis=1)
    device_ids = jnp.arange(N_DP, dtype=jnp.int32)
    target = device_ids
    matched = jnp.zeros((N_DP,), jnp.bool_)
    for bit_index in range(N_DP.bit_length() - 1):
        partner = jnp.bitwise_xor(device_ids, 1 << bit_index)
        picked = ~matched & ~matched[partner] & (loads - loads[partner] >= 2)
        target = jnp.where(picked, partner, target)
        matched = matched | picked | picked[partner]
    pick_index = jax.random.randint(jax.random.fold_in(key, 102), (N_DP,), 0, loads, jnp.int32)
    starts = jnp.cumsum(blocks, axis=1) - blocks
    inside = (pick_index[:, None] >= starts) & (pick_index[:, None] < starts + blocks)
    offsets = jnp.arange(REQ_DEV, dtype=jnp.int32)[None, :] * MAXB + pick_index[:, None] - starts
    slot_id = jnp.sum(jnp.where(inside, offsets, 0), axis=1)
    slot_id = jnp.where(target != device_ids, slot_id, 0)
    return jnp.stack([target, slot_id], axis=1).astype(jnp.int32)


def touch_ends(entries, rng, least, high):
    longest = entries.shape.index(max(entries.shape))
    spots = []
    for shift in (0, 1):
        where = [jax.random.randint(jax.random.fold_in(rng, axis), (), 0, length) for axis, length in enumerate(entries.shape)]
        where[longest] = (where[longest] + shift) % entries.shape[longest]
        spots.append(tuple(where))
    return entries.at[spots[0]].set(least).at[spots[1]].set(high)


def level_of(rng, shape, pieces, low, largest):
    loudness, own = 1.0, jax.random.fold_in(rng, 6)
    for axis_at, shards_of in pieces:
        heights = jnp.exp(jax.random.uniform(jax.random.fold_in(own, axis_at), (shards_of,), jnp.float32, low / len(pieces), largest / len(pieces)))
        loudness = loudness * jnp.repeat(heights, shape[axis_at] // shards_of).reshape([-1 if axis == axis_at else 1 for axis in range(len(shape))])
    return loudness


def normal_values(rng, shape, scale, most, pieces=(), kind=jnp.bfloat16):
    gain = level_of(rng, shape, pieces, -0.22, 0.18) if pieces else 1.0
    array = jax.random.normal(rng, shape, jnp.float32) * scale * gain
    return jnp.minimum(jnp.maximum(array, -most), most).astype(kind)


def setup_inputs(seed: int = 0) -> dict:
    seeds = jax.random.split(jax.random.key(seed), 9)
    queries = draw_queries(jax.random.fold_in(seeds[8], 71), 0)
    draft_key_value = normal_values(seeds[1], (REQUEST_COUNT, 2, TREE_ROWS, KEY_VALUE_HEADS * HEAD_SIZE), 1.0, 4.5, ((0, 8), (3, 4)))
    cache_kv = draw_cache_kv(jax.random.fold_in(seeds[8], 71), 0)
    out_weight = normal_values(seeds[3], (QUERY_HEADS * HEAD_SIZE, D), (QUERY_HEADS * HEAD_SIZE) ** -0.5, 0.109375, ((0, 4),))
    tree_sizes = draw_tree_sizes(jax.random.fold_in(seeds[8], 71), 0)
    parents = draw_parents(jax.random.fold_in(seeds[8], 71), 0)
    cache_lens = touch_ends(jax.random.randint(seeds[6], (REQUEST_COUNT,), CACHE_SLOTS // 4, CACHE_SLOTS + 1), jax.random.fold_in(seeds[6], 1), CACHE_SLOTS // 4, CACHE_SLOTS).astype(jnp.int32)
    block_moves = draw_block_moves(jax.random.fold_in(seeds[8], 71), 0)
    return dict(queries=queries, draft_key_value=draft_key_value, cache_kv=cache_kv, out_weight=out_weight, tree_sizes=tree_sizes, parents=parents, cache_lens=cache_lens, block_moves=block_moves)


def ancestry(parent_row):
    node_count = parent_row.shape[0]
    position = jnp.arange(node_count, dtype=jnp.int32)
    reached = (position[:, None] == position[None, :]) | (parent_row[:, None] == position[None, :])
    jumper = parent_row
    for doubling in range(max(node_count - 1, 1).bit_length()):
        reached = reached | reached[jumper]
        jumper = jumper[jumper]
    return reached


def attend_request(packed):
    query_matrix, draft_pair, stored_pair, parent_row, tree_size, cache_length = packed
    heads_per_group = QUERY_HEADS // KEY_VALUE_HEADS
    score_scale = HEAD_SIZE ** -0.5
    query_head_rows = query_matrix.astype(jnp.float32).reshape(TREE_ROWS, KEY_VALUE_HEADS, heads_per_group, HEAD_SIZE)
    stored_keys = stored_pair[0].astype(jnp.float32).reshape(CACHE_SLOTS, KEY_VALUE_HEADS, HEAD_SIZE)
    stored_values = stored_pair[1].astype(jnp.float32).reshape(CACHE_SLOTS, KEY_VALUE_HEADS, HEAD_SIZE)
    draft_keys = draft_pair[0].astype(jnp.float32).reshape(TREE_ROWS, KEY_VALUE_HEADS, HEAD_SIZE)
    draft_values = draft_pair[1].astype(jnp.float32).reshape(TREE_ROWS, KEY_VALUE_HEADS, HEAD_SIZE)
    cache_scores = jnp.einsum("ngrd,cgd->ngrc", query_head_rows, stored_keys) * score_scale
    tree_scores = jnp.einsum("ngrd,jgd->ngrj", query_head_rows, draft_keys) * score_scale
    cache_open = jnp.arange(CACHE_SLOTS, dtype=jnp.int32) < cache_length
    tree_open = ancestry(parent_row)
    cache_scores = jnp.where(cache_open[None, None, None, :], cache_scores, -jnp.inf)
    tree_scores = jnp.where(tree_open[:, None, None, :], tree_scores, -jnp.inf)
    highest = jnp.maximum(jnp.max(cache_scores, axis=-1), jnp.max(tree_scores, axis=-1))[..., None]
    cache_exp = jnp.exp(cache_scores - highest)
    tree_exp = jnp.exp(tree_scores - highest)
    denominator = jnp.sum(cache_exp, axis=-1, keepdims=True) + jnp.sum(tree_exp, axis=-1, keepdims=True)
    cache_weights = lax.optimization_barrier((cache_exp / denominator).astype(jnp.bfloat16)).astype(jnp.float32)
    tree_weights = lax.optimization_barrier((tree_exp / denominator).astype(jnp.bfloat16)).astype(jnp.float32)
    blended = jnp.einsum("ngrc,cgd->ngrd", cache_weights, stored_values)
    blended = blended + jnp.einsum("ngrj,jgd->ngrd", tree_weights, draft_values)
    live_rows = (jnp.arange(TREE_ROWS, dtype=jnp.int32) < tree_size).astype(jnp.float32)
    blended = blended.reshape(TREE_ROWS, QUERY_HEADS * HEAD_SIZE) * live_rows[:, None]
    return blended.astype(jnp.bfloat16)


def project(rows, out_weight):
    group_width = rows.shape[1] // N_TENSOR

    def one_block(row_block):
        summed = jnp.zeros((row_block.shape[0], out_weight.shape[1]), jnp.float32)
        for head_group in range(N_TENSOR):
            lower = head_group * group_width
            group_part = jnp.dot(row_block[:, lower:lower + group_width], out_weight[lower:lower + group_width], preferred_element_type=jnp.float32)
            summed = summed + lax.optimization_barrier(group_part.astype(jnp.bfloat16)).astype(jnp.float32)
        return summed.astype(jnp.bfloat16)

    mapped = lax.map(one_block, rows.reshape(-1, BLK, rows.shape[1]))
    return mapped.reshape(rows.shape[0], out_weight.shape[1])


def reference(queries, draft_key_value, cache_kv, out_weight, tree_sizes, parents, cache_lens, block_moves):
    attn = lax.map(attend_request, (queries, draft_key_value, cache_kv, parents, tree_sizes, cache_lens))
    device_ids = jnp.arange(N_DP, dtype=jnp.int32)
    target = block_moves[:, 0]
    chosen = block_moves[:, 1]
    sending = target != device_ids
    slot_grid = jnp.arange(REQ_DEV * MAXB, dtype=jnp.int32).reshape(1, REQ_DEV, MAXB)
    moved_away = (sending[:, None, None] & (chosen[:, None, None] == slot_grid)).reshape(REQUEST_COUNT, MAXB)
    blocks = attn.reshape(REQUEST_COUNT, MAXB, BLK, QUERY_HEADS * HEAD_SIZE)
    kept = jnp.where(moved_away[:, :, None, None], jnp.zeros_like(blocks), blocks)
    arrives = sending[None, :] & (target[None, :] == device_ids[:, None])
    present = jnp.any(arrives, axis=1)
    source = jnp.sum(jnp.where(arrives, device_ids[None, :], 0), axis=1).astype(jnp.int32)
    by_device = blocks.reshape(N_DP, REQ_DEV * MAXB, BLK, QUERY_HEADS * HEAD_SIZE)
    picked = by_device[source, chosen[source]]
    arrived = jnp.where(present[:, None, None], picked, jnp.zeros_like(picked))
    own_out = project(kept.reshape(REQUEST_COUNT * TREE_ROWS, QUERY_HEADS * HEAD_SIZE), out_weight)
    moved_out = project(arrived.reshape(N_DP * BLK, QUERY_HEADS * HEAD_SIZE), out_weight)
    return (own_out, moved_out)
```

```python
import functools
import math

import jax
import jax.numpy as jnp
from jax import lax
from jax.experimental import pallas as pl
from jax.experimental.pallas import tpu as pltpu
from jax.sharding import PartitionSpec as P

HEAD_SIZE = 128
BLK = 128
SCALE = HEAD_SIZE**-0.5 * math.log2(math.e)
LOW = -1e30
CHUNK = 512
TILES = 3
PIECES = 4


def swapped(array, axis, bit):
    return lax.ppermute(array, axis, [(i, i ^ bit) for i in range(lax.axis_size(axis))])


def reach_kernel(parent_ref, bias_ref, reach_ref):
    requests, nodes, _ = reach_ref.shape
    for r in range(requests):
        up = parent_ref[r]
        for b in range(nodes // BLK):
            rows = pl.ds(b * BLK, BLK)
            mine = up[b * BLK : (b + 1) * BLK]
            row = lax.broadcasted_iota(jnp.int32, (BLK, BLK), 0)
            column = lax.broadcasted_iota(jnp.int32, (BLK, BLK), 1)
            linked = (row == column) | (mine == column + b * BLK)
            inside = jnp.where(linked, 1.0, 0.0).astype(jnp.bfloat16)
            for _ in range((BLK - 1).bit_length()):
                squared = jnp.dot(inside, inside, preferred_element_type=jnp.float32)
                inside = jnp.where(squared > 0.5, 1.0, 0.0).astype(jnp.bfloat16)
            reach_ref[r, rows, :] = jnp.zeros((BLK, nodes), jnp.bfloat16)
            if b:
                before = lax.broadcasted_iota(jnp.int32, (BLK, b * BLK), 1)
                step = jnp.where(mine == before, 1.0, 0.0).astype(jnp.bfloat16)
                outer = jnp.dot(
                    step, reach_ref[r, : b * BLK, : b * BLK], preferred_element_type=jnp.float32
                ).astype(jnp.bfloat16)
                reach_ref[r, rows, : b * BLK] = jnp.dot(
                    inside, outer, preferred_element_type=jnp.float32
                ).astype(jnp.bfloat16)
            reach_ref[r, rows, b * BLK : (b + 1) * BLK] = inside
        bias_ref[r] = jnp.where(reach_ref[r].astype(jnp.float32) > 0.5, 0.0, LOW)


def reach_bias(parents):
    requests, nodes = parents.shape
    return pl.pallas_call(
        reach_kernel,
        out_shape=jax.ShapeDtypeStruct((requests, nodes, nodes), jnp.float32),
        scratch_shapes=[pltpu.VMEM((requests, nodes, nodes), jnp.bfloat16)],
        cost_estimate=pl.CostEstimate(
            flops=10**9, bytes_accessed=4 * requests * nodes * nodes, transcendentals=0
        ),
        name="reach",
    )(parents[:, :, None])


def attend_kernel(
    meta_ref, q_ref, draft_ref, cache_ref, bias_ref, out_ref, stack_ref, top_ref, total_ref
):
    step = pl.program_id(0)
    block = meta_ref[1, step]
    size = meta_ref[2, step]
    length = meta_ref[3, step]
    active = meta_ref[4, step]
    heads = q_ref.shape[2] // HEAD_SIZE
    rows = heads * BLK
    tile = rows // TILES
    slots = cache_ref.shape[2]
    nodes = draft_ref.shape[2]

    def scores(at, keys):
        return (
            lax.dot_general(
                stack_ref[pl.ds(at, tile), :],
                keys,
                (((1,), (1,)), ((), ())),
                preferred_element_type=jnp.float32,
            )
            * SCALE
        )

    def widened(values):
        return jnp.concatenate([values, jnp.ones(values.shape, values.dtype)], axis=1)

    def tree(width):
        keys = draft_ref[0, 0, :width, :]
        values = widened(draft_ref[0, 1, :width, :])
        bias = bias_ref[0, :, :width]
        bias = jnp.concatenate([bias] * (tile // BLK), axis=0)
        for part in range(TILES):
            at = part * tile
            s = scores(at, keys) + bias
            top = jnp.max(s, axis=1, keepdims=True)
            p = jnp.exp2(s - top).astype(jnp.bfloat16)
            top_ref[pl.ds(at, tile), :] = jnp.broadcast_to(top, (tile, HEAD_SIZE))
            total_ref[pl.ds(at, tile), :] = jnp.dot(p, values, preferred_element_type=jnp.float32)

    @pl.when(active == 0)
    def _():
        out_ref[...] = jnp.zeros_like(out_ref)

    @pl.when(active != 0)
    def _():
        for head in range(heads):
            stack_ref[head * BLK : (head + 1) * BLK, :] = q_ref[
                0, :, head * HEAD_SIZE : (head + 1) * HEAD_SIZE
            ]
        half = nodes // 2

        @pl.when((block + 1) * BLK <= half)
        def _():
            tree(half)

        @pl.when((block + 1) * BLK > half)
        def _():
            tree(nodes)

        def chunk(index, _):
            first = index * CHUNK
            start = pl.multiple_of(jnp.minimum(first, slots - CHUNK), BLK)
            keys = cache_ref[0, 0, pl.ds(start, CHUNK), :]
            values = widened(cache_ref[0, 1, pl.ds(start, CHUNK), :])
            position = lax.broadcasted_iota(jnp.int32, (1, CHUNK), 1) + start
            bias = jnp.where((position >= first) & (position < length), 0.0, LOW)
            for part in range(TILES):
                at = part * tile
                s = scores(at, keys) + bias
                old = top_ref[pl.ds(at, tile), :][:, :1]
                top = jnp.maximum(old, jnp.max(s, axis=1, keepdims=True))
                p = jnp.exp2(s - top).astype(jnp.bfloat16)
                shrink = jnp.exp2(old - top)
                top_ref[pl.ds(at, tile), :] = jnp.broadcast_to(top, (tile, HEAD_SIZE))
                total_ref[pl.ds(at, tile), :] = total_ref[pl.ds(at, tile), :] * shrink + jnp.dot(
                    p, values, preferred_element_type=jnp.float32
                )
            return 0

        lax.fori_loop(0, (length + CHUNK - 1) // CHUNK, chunk, 0)
        live = block * BLK + lax.broadcasted_iota(jnp.int32, (BLK, HEAD_SIZE), 0) < size
        for head in range(heads):
            at = head * BLK
            result = total_ref[at : at + BLK, :HEAD_SIZE] / total_ref[at : at + BLK, HEAD_SIZE:]
            out_ref[:, head * HEAD_SIZE : (head + 1) * HEAD_SIZE] = jnp.where(
                live, result, 0.0
            ).astype(out_ref.dtype)


def attend(meta, queries, draft, cache, bias, name):
    steps = meta.shape[1]
    width = queries.shape[2]
    nodes = draft.shape[2]
    slots = cache.shape[2]
    rows = width // HEAD_SIZE * BLK
    grid_spec = pltpu.PrefetchScalarGridSpec(
        num_scalar_prefetch=1,
        grid=(steps,),
        in_specs=[
            pl.BlockSpec((1, BLK, width), lambda s, m: (m[0, s], m[1, s], 0)),
            pl.BlockSpec((1, 2, nodes, HEAD_SIZE), lambda s, m: (m[0, s], 0, 0, 0)),
            pl.BlockSpec((1, 2, slots, HEAD_SIZE), lambda s, m: (m[0, s], 0, 0, 0)),
            pl.BlockSpec((1, BLK, nodes), lambda s, m: (m[0, s], m[1, s], 0)),
        ],
        out_specs=pl.BlockSpec((BLK, width), lambda s, m: (s, 0)),
        scratch_shapes=[
            pltpu.VMEM((rows, HEAD_SIZE), jnp.bfloat16),
            pltpu.VMEM((rows, HEAD_SIZE), jnp.float32),
            pltpu.VMEM((rows, 2 * HEAD_SIZE), jnp.float32),
        ],
    )
    return pl.pallas_call(
        attend_kernel,
        out_shape=jax.ShapeDtypeStruct((steps * BLK, width), queries.dtype),
        grid_spec=grid_spec,
        cost_estimate=pl.CostEstimate(
            flops=steps * rows * (nodes + slots) * HEAD_SIZE * 4,
            bytes_accessed=4 * (nodes + slots) * HEAD_SIZE * 2 + steps * BLK * width * 4,
            transcendentals=steps * rows * (nodes + slots),
        ),
        name=name,
    )(meta, queries, draft, cache, bias)


def local(
    queries, draft_key_value, cache_kv, out_weight, tree_sizes, parents, cache_lens, block_moves
):
    requests, nodes, width = queries.shape
    blocks = nodes // BLK
    dp_count = lax.axis_size("dp")
    mine = lax.axis_index("dp")
    tensor_count = lax.axis_size("tensor")
    spot = lax.axis_index("tensor")
    pairs = tensor_count // 2
    high, low = spot // 2, spot % 2
    first = mine * requests
    sizes = lax.dynamic_slice_in_dim(tree_sizes, first, requests, 0)
    lengths = lax.dynamic_slice_in_dim(cache_lens, first, requests, 0)
    own_parents = lax.dynamic_slice_in_dim(parents, first, requests, 0)
    target, chosen = block_moves[:, 0], block_moves[:, 1]
    sending = block_moves[mine, 0] != mine
    my_slot = block_moves[mine, 1]
    ids = jnp.arange(dp_count, dtype=jnp.int32)
    arrives = (target == mine) & (target != ids)
    present = jnp.any(arrives)
    bits = jnp.bitwise_xor(jnp.sum(jnp.where(arrives, ids, 0)), mine)

    sibling_weight = swapped(out_weight, "tensor", 1)
    bias = reach_bias(own_parents)

    def meta_of(slot, wanted):
        request, block = slot // blocks, slot % blocks
        size = sizes[request]
        active = wanted & (block * BLK < size)
        return jnp.stack(
            [request, block, size, lengths[request], active.astype(jnp.int32)]
        ).astype(jnp.int32)

    given = attend(
        meta_of(my_slot[None], sending[None]), queries, draft_key_value, cache_kv, bias, "given"
    )
    arrived = jnp.zeros_like(given)
    for bit in range(dp_count.bit_length() - 1):
        fresh = swapped(given, "dp", 1 << bit)
        arrived = jnp.where(present & (bits == 1 << bit), fresh, arrived)
    arrived = arrived.reshape(tensor_count, -1, width)

    per_pair = requests * blocks // pairs

    def rows_of(part):
        slot = part * per_pair + jnp.arange(per_pair, dtype=jnp.int32)
        keep = jnp.logical_not(sending & (slot == my_slot))
        rows = attend(
            meta_of(slot, keep), queries, draft_key_value, cache_kv, bias, "kept"
        ).reshape(2, -1, width)
        new = lax.dynamic_slice_in_dim(arrived, part * 2, 2, 0)
        both = jnp.concatenate([rows, new], axis=1)
        ours = lax.dynamic_index_in_dim(both, low, 0, keepdims=False)
        theirs = lax.dynamic_index_in_dim(both, 1 - low, 0, keepdims=False)
        return ours, swapped(theirs, "tensor", 1)

    columns = out_weight.shape[1] // PIECES

    def product(ours, theirs, piece):
        at = slice(piece * columns, (piece + 1) * columns)
        total = jnp.dot(ours, out_weight[:, at], preferred_element_type=jnp.float32)
        return total + jnp.dot(theirs, sibling_weight[:, at], preferred_element_type=jnp.float32)

    coming = [[] for _ in range(PIECES)]
    for hop in range(1, pairs):
        ours, theirs = rows_of((high + hop) % pairs)
        ring = [
            (2 * h + l, 2 * ((h + hop) % pairs) + l) for h in range(pairs) for l in range(2)
        ]
        for piece in range(PIECES):
            part = product(ours, theirs, piece).astype(jnp.bfloat16)
            coming[piece].append(lax.ppermute(part, "tensor", ring))
    ours, theirs = rows_of(high)
    done = []
    for piece in range(PIECES):
        total = product(ours, theirs, piece)
        for part in coming[piece]:
            total = total + part.astype(jnp.float32)
        done.append(total.astype(jnp.bfloat16))
    share = nodes * requests // tensor_count
    own_out = jnp.concatenate([part[:share] for part in done], axis=1)
    moved_out = jnp.concatenate([part[share:] for part in done], axis=1)
    return own_out, moved_out


def solution(mesh):
    in_specs = (
        P("dp", None, "tensor"),
        P("dp", None, None, "tensor"),
        P("dp", None, None, "tensor"),
        P("tensor", None),
        P(),
        P(),
        P(),
        P(),
    )
    out_specs = (P(("dp", "tensor"), None), P(("dp", "tensor"), None))
    return jax.shard_map(local, mesh=mesh, in_specs=in_specs, out_specs=out_specs, check_vma=False)
```

```python
import functools
import math

import jax
import jax.numpy as jnp
from jax import lax
from jax.experimental import pallas as pl
from jax.experimental.pallas import tpu as pltpu
from jax.sharding import PartitionSpec as P


HEAD_SIZE = 128
BLK = 128
SCALE = HEAD_SIZE**-0.5 * math.log2(math.e)
LOW = -1e30
CHUNK = 512
TILES = 3
PIECES = 2


def swapped(array, axis, bit):
    return lax.ppermute(array, axis, [(i, i ^ bit) for i in range(lax.axis_size(axis))])


def reach_kernel(ids_ref, parent_ref, bias_ref, reach_ref):
    requests, nodes, _ = reach_ref.shape
    blocks = nodes // BLK
    spots = [(r, b) for r in range(requests) for b in range(blocks)]
    row = lax.broadcasted_iota(jnp.int32, (BLK, BLK), 0)
    column = lax.broadcasted_iota(jnp.int32, (BLK, BLK), 1)
    ups, insides = {}, {}
    for r, b in spots:
        up = parent_ref[0, r : r + 1, b * BLK : (b + 1) * BLK]
        ups[r, b] = jnp.broadcast_to(up, (BLK, BLK)).T
        linked = (row == column) | (ups[r, b] == column + b * BLK)
        insides[r, b] = jnp.where(linked, 1.0, 0.0).astype(jnp.bfloat16)
    for _ in range((BLK - 1).bit_length()):
        for at in spots:
            squared = jnp.dot(insides[at], insides[at], preferred_element_type=jnp.float32)
            insides[at] = jnp.where(squared > 0.5, 1.0, 0.0).astype(jnp.bfloat16)
    for b in range(blocks):
        for r in range(requests):
            rows = pl.ds(b * BLK, BLK)
            for k in range(blocks):
                if k >= b:
                    part = insides[r, b] if k == b else jnp.zeros((BLK, BLK), jnp.bfloat16)
                    reach_ref[r, rows, k * BLK : (k + 1) * BLK] = part
            if b:
                steps = [ups[r, b] == column + k * BLK for k in range(b)]
                step = jnp.concatenate(
                    [jnp.where(one, 1.0, 0.0).astype(jnp.bfloat16) for one in steps], axis=1
                )
                outer = jnp.dot(
                    step, reach_ref[r, : b * BLK, : b * BLK], preferred_element_type=jnp.float32
                ).astype(jnp.bfloat16)
                reach_ref[r, rows, : b * BLK] = jnp.dot(
                    insides[r, b], outer, preferred_element_type=jnp.float32
                ).astype(jnp.bfloat16)
            bias_ref[r, rows, :] = jnp.where(
                reach_ref[r, rows, :].astype(jnp.float32) > 0.5, 0.0, LOW
            )


def reach_bias(ids, parents, requests):
    nodes = parents.shape[1]
    return pl.pallas_call(
        reach_kernel,
        out_shape=jax.ShapeDtypeStruct((requests, nodes, nodes), jnp.float32),
        grid_spec=pltpu.PrefetchScalarGridSpec(
            num_scalar_prefetch=1,
            grid=(1,),
            in_specs=[pl.BlockSpec((1, requests, nodes), lambda s, m: (m[0], 0, 0))],
            out_specs=pl.BlockSpec((requests, nodes, nodes), lambda s, m: (0, 0, 0)),
            scratch_shapes=[pltpu.VMEM((requests, nodes, nodes), jnp.bfloat16)],
        ),
        cost_estimate=pl.CostEstimate(
            flops=10**9, bytes_accessed=4 * requests * nodes * nodes, transcendentals=0
        ),
        name="reach",
    )(ids, parents.reshape(-1, requests, nodes))


def attend_kernel(
    slot_of,
    given,
    ids_ref,
    sizes_ref,
    lengths_ref,
    moves_ref,
    q_ref,
    draft_ref,
    cache_ref,
    bias_ref,
    after_ref,
    out_ref,
    stack_ref,
    top_ref,
    total_ref,
):
    blocks = draft_ref.shape[2] // BLK
    step = pl.program_id(0)
    slot = slot_of(step, ids_ref, moves_ref)
    mine = ids_ref[0]
    request, block = slot // blocks, slot % blocks
    per_device = sizes_ref.shape[0] // moves_ref.shape[0]
    size = sizes_ref[mine * per_device + request]
    length = lengths_ref[mine * per_device + request]
    moved = (moves_ref[mine, 0] != mine) & (moves_ref[mine, 1] == slot)
    wanted = moved == (step >= given)
    active = (wanted & (block * BLK < size)).astype(jnp.int32)
    heads = q_ref.shape[2] // HEAD_SIZE
    rows = heads * BLK
    tile = rows // TILES
    slots = cache_ref.shape[2]
    nodes = draft_ref.shape[2]

    def scores(at, keys):
        return (
            lax.dot_general(
                stack_ref[pl.ds(at, tile), :],
                keys,
                (((1,), (1,)), ((), ())),
                preferred_element_type=jnp.float32,
            )
            * SCALE
        )

    def widened(values):
        return jnp.concatenate([values, jnp.ones(values.shape, values.dtype)], axis=1)

    def tree(width):
        keys = draft_ref[0, 0, :width, :]
        values = widened(draft_ref[0, 1, :width, :])
        bias = bias_ref[0, :, :width]
        bias = jnp.concatenate([bias] * (tile // BLK), axis=0)
        for part in range(TILES):
            at = part * tile
            s = scores(at, keys) + bias
            top = jnp.max(s, axis=1, keepdims=True)
            p = jnp.exp2(s - top).astype(jnp.bfloat16)
            top_ref[pl.ds(at, tile), :] = jnp.broadcast_to(top, (tile, HEAD_SIZE))
            total_ref[pl.ds(at, tile), :] = jnp.dot(p, values, preferred_element_type=jnp.float32)

    @pl.when(active == 0)
    def _():
        out_ref[...] = jnp.zeros_like(out_ref)

    @pl.when(active != 0)
    def _():
        for head in range(heads):
            stack_ref[head * BLK : (head + 1) * BLK, :] = q_ref[
                0, :, head * HEAD_SIZE : (head + 1) * HEAD_SIZE
            ]
        half = nodes // 2

        @pl.when((block + 1) * BLK <= half)
        def _():
            tree(half)

        @pl.when((block + 1) * BLK > half)
        def _():
            tree(nodes)

        def chunk(index, _):
            first = index * CHUNK
            start = pl.multiple_of(jnp.minimum(first, slots - CHUNK), BLK)
            keys = cache_ref[0, 0, pl.ds(start, CHUNK), :]
            values = widened(cache_ref[0, 1, pl.ds(start, CHUNK), :])
            position = lax.broadcasted_iota(jnp.int32, (1, CHUNK), 1) + start
            bias = jnp.where((position >= first) & (position < length), 0.0, LOW)
            for part in range(TILES):
                at = part * tile
                s = scores(at, keys) + bias
                old = top_ref[pl.ds(at, tile), :][:, :1]
                top = jnp.maximum(old, jnp.max(s, axis=1, keepdims=True))
                p = jnp.exp2(s - top).astype(jnp.bfloat16)
                shrink = jnp.exp2(old - top)
                top_ref[pl.ds(at, tile), :] = jnp.broadcast_to(top, (tile, HEAD_SIZE))
                total_ref[pl.ds(at, tile), :] = total_ref[pl.ds(at, tile), :] * shrink + jnp.dot(
                    p, values, preferred_element_type=jnp.float32
                )
            return 0

        lax.fori_loop(0, (length + CHUNK - 1) // CHUNK, chunk, 0)
        live = block * BLK + lax.broadcasted_iota(jnp.int32, (BLK, HEAD_SIZE), 0) < size
        for head in range(heads):
            at = head * BLK
            result = total_ref[at : at + BLK, :HEAD_SIZE] / total_ref[at : at + BLK, HEAD_SIZE:]
            out_ref[:, head * HEAD_SIZE : (head + 1) * HEAD_SIZE] = jnp.where(
                live, result, 0.0
            ).astype(out_ref.dtype)


def attend(scalars, slot_of, steps, given, queries, draft, cache, bias, after):
    width = queries.shape[2]
    nodes = draft.shape[2]
    slots = cache.shape[2]
    blocks = nodes // BLK
    rows = width // HEAD_SIZE * BLK

    def request(s, ids, sizes, lengths, moves):
        return slot_of(s, ids, moves) // blocks, 0, 0, 0

    def rows_at(s, ids, sizes, lengths, moves):
        slot = slot_of(s, ids, moves)
        return slot // blocks, slot % blocks, 0

    grid_spec = pltpu.PrefetchScalarGridSpec(
        num_scalar_prefetch=4,
        grid=(steps,),
        in_specs=[
            pl.BlockSpec((1, BLK, width), rows_at),
            pl.BlockSpec((1, 2, nodes, HEAD_SIZE), request),
            pl.BlockSpec((1, 2, slots, HEAD_SIZE), request),
            pl.BlockSpec((1, BLK, nodes), rows_at),
            pl.BlockSpec(memory_space=pl.ANY),
        ],
        out_specs=pl.BlockSpec((BLK, width), lambda s, *_: (s, 0)),
        scratch_shapes=[
            pltpu.VMEM((rows, HEAD_SIZE), jnp.bfloat16),
            pltpu.VMEM((rows, HEAD_SIZE), jnp.float32),
            pltpu.VMEM((rows, 2 * HEAD_SIZE), jnp.float32),
        ],
    )
    return pl.pallas_call(
        functools.partial(attend_kernel, slot_of, given),
        out_shape=jax.ShapeDtypeStruct((steps * BLK, width), queries.dtype),
        grid_spec=grid_spec,
        cost_estimate=pl.CostEstimate(
            flops=steps * rows * (nodes + slots) * HEAD_SIZE * 4,
            bytes_accessed=4 * (nodes + slots) * HEAD_SIZE * 2 + steps * BLK * width * 4,
            transcendentals=steps * rows * (nodes + slots),
        ),
    )(*scalars, queries, draft, cache, bias, after)


def local(
    queries, draft_key_value, cache_kv, out_weight, tree_sizes, parents, cache_lens, block_moves
):
    requests, nodes, width = queries.shape
    blocks = nodes // BLK
    dp_count = lax.axis_size("dp")
    mine = lax.axis_index("dp")
    tensor_count = lax.axis_size("tensor")
    spot = lax.axis_index("tensor")
    pairs = tensor_count // 2
    high, low = spot // 2, spot % 2
    ids = jnp.stack([mine, high, low]).astype(jnp.int32)
    scalars = (ids, tree_sizes, cache_lens, block_moves)
    sibling_weight = swapped(out_weight, "tensor", 1)
    bias = reach_bias(ids, parents, requests)
    per_pair = requests * blocks // pairs
    per_core = per_pair // 2

    def cores_share(rows):
        ours = lax.dynamic_index_in_dim(rows, low, 0, keepdims=False)
        theirs = lax.dynamic_index_in_dim(rows, 1 - low, 0, keepdims=False)
        return ours, swapped(theirs, "tensor", 1)

    def kept_rows(hop, first, count, giving, after):
        def slot_of(s, ids, moves):
            part = (ids[1] + hop) % pairs
            slot = part * per_pair + (s // count) * per_core + first + s % count
            return jnp.where(s >= 2 * count, moves[ids[0], 1], slot)

        rows = attend(
            scalars, slot_of, 2 * count + giving, 2 * count, queries, draft_key_value,
            cache_kv, bias, after,
        )
        split = 2 * count * BLK
        return cores_share(rows[:split].reshape(2, count * BLK, width)), rows[split:]

    def product(rows, piece, pieces):
        columns = out_weight.shape[1] // pieces
        at = slice(piece * columns, (piece + 1) * columns)
        ours, theirs = rows
        total = jnp.dot(ours, out_weight[:, at], preferred_element_type=jnp.float32)
        return total + jnp.dot(theirs, sibling_weight[:, at], preferred_element_type=jnp.float32)

    def onward(part, hop):
        ring = [
            (2 * h + l, 2 * ((h + hop) % pairs) + l) for h in range(pairs) for l in range(2)
        ]
        return lax.ppermute(part, "tensor", ring)

    coming = {}
    after = bias
    for hop in range(1, pairs):
        for sub in range(per_core):
            giving = int((hop, sub) == (1, per_core - 1))
            rows, given = kept_rows(hop, sub, 1, giving, after)
            for piece in range(PIECES):
                part = product(rows, piece, PIECES).astype(jnp.bfloat16)
                coming.setdefault((sub, piece), []).append(onward(part, hop))
            after = part
            if giving:
                target = block_moves[:, 0]
                numbers = jnp.arange(dp_count, dtype=jnp.int32)
                arrives = (target == mine) & (target != numbers)
                present = jnp.any(arrives)
                bits = jnp.bitwise_xor(jnp.sum(jnp.where(arrives, numbers, 0)), mine)
                arrived = jnp.zeros_like(given)
                for bit in range(dp_count.bit_length() - 1):
                    fresh = swapped(given, "dp", 1 << bit)
                    arrived = jnp.where(present & (bits == 1 << bit), fresh, arrived)
                arrived = arrived.reshape(pairs, 2, -1, width)
    ours, _ = kept_rows(0, 0, per_core, 0, after)

    def new_rows(hop):
        part = lax.dynamic_index_in_dim(arrived, (high + hop) % pairs, 0, keepdims=False)
        return cores_share(part)

    new_coming = [
        onward(product(new_rows(hop), 0, 1).astype(jnp.bfloat16), hop)
        for hop in range(1, pairs)
    ]

    def total_of(rows, piece, pieces, parts):
        total = lax.optimization_barrier(product(rows, piece, pieces))
        for part in parts:
            total = total + part.astype(jnp.float32)
        return total.astype(jnp.bfloat16)

    done = []
    for sub in range(per_core):
        rows = tuple(one[sub * BLK : (sub + 1) * BLK] for one in ours)
        pieces = [total_of(rows, piece, PIECES, coming[sub, piece]) for piece in range(PIECES)]
        done.append(jnp.concatenate(pieces, axis=1))
    own_out = jnp.concatenate(done, axis=0)
    moved_out = total_of(new_rows(0), 0, 1, new_coming)
    return own_out, moved_out


def solution(mesh):
    in_specs = (
        P("dp", None, "tensor"),
        P("dp", None, None, "tensor"),
        P("dp", None, None, "tensor"),
        P("tensor", None),
        P(),
        P(),
        P(),
        P(),
    )
    out_specs = (P(("dp", "tensor"), None), P(("dp", "tensor"), None))

    def build(queries, *rest):
        step = jax.shard_map(
            local, mesh=mesh, in_specs=in_specs, out_specs=out_specs, check_vma=False
        )
        return step(queries, *rest)

    return build
```

```python
import functools
import math

import jax
import jax.numpy as jnp
from jax import lax
from jax.experimental import pallas as pl
from jax.experimental.pallas import tpu as pltpu
from jax.sharding import PartitionSpec as P


HEAD_SIZE = 128
BLK = 128
SCALE = HEAD_SIZE**-0.5 * math.log2(math.e)
LOW = -1e30
CHUNK = 512
TILES = 3
COLUMNS = 512


def swapped(array, axis, bit):
    return lax.ppermute(array, axis, [(i, i ^ bit) for i in range(lax.axis_size(axis))])


def reach_kernel(ids_ref, parent_ref, bias_ref, reach_ref):
    requests, nodes, _ = reach_ref.shape
    blocks = nodes // BLK
    spots = [(r, b) for r in range(requests) for b in range(blocks)]
    row = lax.broadcasted_iota(jnp.int32, (BLK, BLK), 0)
    column = lax.broadcasted_iota(jnp.int32, (BLK, BLK), 1)
    ups, insides = {}, {}
    for r, b in spots:
        up = parent_ref[0, r : r + 1, b * BLK : (b + 1) * BLK]
        ups[r, b] = jnp.broadcast_to(up, (BLK, BLK)).T
        linked = (row == column) | (ups[r, b] == column + b * BLK)
        insides[r, b] = jnp.where(linked, 1.0, 0.0).astype(jnp.bfloat16)
    for _ in range((BLK - 1).bit_length()):
        for at in spots:
            squared = jnp.dot(insides[at], insides[at], preferred_element_type=jnp.float32)
            insides[at] = jnp.where(squared > 0.5, 1.0, 0.0).astype(jnp.bfloat16)
    for b in range(blocks):
        for r in range(requests):
            rows = pl.ds(b * BLK, BLK)
            for k in range(blocks):
                if k >= b:
                    part = insides[r, b] if k == b else jnp.zeros((BLK, BLK), jnp.bfloat16)
                    reach_ref[r, rows, k * BLK : (k + 1) * BLK] = part
            if b:
                steps = [ups[r, b] == column + k * BLK for k in range(b)]
                step = jnp.concatenate(
                    [jnp.where(one, 1.0, 0.0).astype(jnp.bfloat16) for one in steps], axis=1
                )
                outer = jnp.dot(
                    step, reach_ref[r, : b * BLK, : b * BLK], preferred_element_type=jnp.float32
                ).astype(jnp.bfloat16)
                reach_ref[r, rows, : b * BLK] = jnp.dot(
                    insides[r, b], outer, preferred_element_type=jnp.float32
                ).astype(jnp.bfloat16)
            bias_ref[r, rows, :] = jnp.where(
                reach_ref[r, rows, :].astype(jnp.float32) > 0.5, 0.0, LOW
            )


def reach_bias(ids, parents, requests):
    nodes = parents.shape[1]
    return pl.pallas_call(
        reach_kernel,
        out_shape=jax.ShapeDtypeStruct((requests, nodes, nodes), jnp.float32),
        grid_spec=pltpu.PrefetchScalarGridSpec(
            num_scalar_prefetch=1,
            grid=(1,),
            in_specs=[pl.BlockSpec((1, requests, nodes), lambda s, m: (m[0], 0, 0))],
            out_specs=pl.BlockSpec((requests, nodes, nodes), lambda s, m: (0, 0, 0)),
            scratch_shapes=[pltpu.VMEM((requests, nodes, nodes), jnp.bfloat16)],
        ),
        cost_estimate=pl.CostEstimate(
            flops=10**9, bytes_accessed=4 * requests * nodes * nodes, transcendentals=0
        ),
        name="reach",
    )(ids, parents.reshape(-1, requests, nodes))


def attend_kernel(
    slot_of,
    given,
    ids_ref,
    sizes_ref,
    lengths_ref,
    moves_ref,
    q_ref,
    draft_ref,
    cache_ref,
    bias_ref,
    after_ref,
    out_ref,
    stack_ref,
    top_ref,
    total_ref,
):
    blocks = draft_ref.shape[2] // BLK
    step = pl.program_id(0)
    slot = slot_of(step, ids_ref, moves_ref)
    mine = ids_ref[0]
    request, block = slot // blocks, slot % blocks
    per_device = sizes_ref.shape[0] // moves_ref.shape[0]
    size = sizes_ref[mine * per_device + request]
    length = lengths_ref[mine * per_device + request]
    moved = (moves_ref[mine, 0] != mine) & (moves_ref[mine, 1] == slot)
    wanted = moved == (step >= given)
    active = (wanted & (block * BLK < size)).astype(jnp.int32)
    heads = q_ref.shape[2] // HEAD_SIZE
    rows = heads * BLK
    tile = rows // TILES
    slots = cache_ref.shape[2]
    nodes = draft_ref.shape[2]

    def scores(at, keys):
        return (
            lax.dot_general(
                stack_ref[pl.ds(at, tile), :],
                keys,
                (((1,), (1,)), ((), ())),
                preferred_element_type=jnp.float32,
            )
            * SCALE
        )

    def widened(values):
        return jnp.concatenate([values, jnp.ones(values.shape, values.dtype)], axis=1)

    def tree(width):
        keys = draft_ref[0, 0, :width, :]
        values = widened(draft_ref[0, 1, :width, :])
        bias = bias_ref[0, :, :width]
        bias = jnp.concatenate([bias] * (tile // BLK), axis=0)
        for part in range(TILES):
            at = part * tile
            s = scores(at, keys) + bias
            top = jnp.max(s, axis=1, keepdims=True)
            p = jnp.exp2(s - top).astype(jnp.bfloat16)
            top_ref[pl.ds(at, tile), :] = jnp.broadcast_to(top, (tile, HEAD_SIZE))
            total_ref[pl.ds(at, tile), :] = jnp.dot(p, values, preferred_element_type=jnp.float32)

    @pl.when(active == 0)
    def _():
        out_ref[...] = jnp.zeros_like(out_ref)

    @pl.when(active != 0)
    def _():
        for head in range(heads):
            stack_ref[head * BLK : (head + 1) * BLK, :] = q_ref[
                0, :, head * HEAD_SIZE : (head + 1) * HEAD_SIZE
            ]
        half = nodes // 2

        @pl.when((block + 1) * BLK <= half)
        def _():
            tree(half)

        @pl.when((block + 1) * BLK > half)
        def _():
            tree(nodes)

        def chunk(index, _):
            first = index * CHUNK
            start = pl.multiple_of(jnp.minimum(first, slots - CHUNK), BLK)
            keys = cache_ref[0, 0, pl.ds(start, CHUNK), :]
            values = widened(cache_ref[0, 1, pl.ds(start, CHUNK), :])
            position = lax.broadcasted_iota(jnp.int32, (1, CHUNK), 1) + start
            bias = jnp.where((position >= first) & (position < length), 0.0, LOW)
            for part in range(TILES):
                at = part * tile
                s = scores(at, keys) + bias
                old = top_ref[pl.ds(at, tile), :][:, :1]
                top = jnp.maximum(old, jnp.max(s, axis=1, keepdims=True))
                p = jnp.exp2(s - top).astype(jnp.bfloat16)
                shrink = jnp.exp2(old - top)
                top_ref[pl.ds(at, tile), :] = jnp.broadcast_to(top, (tile, HEAD_SIZE))
                total_ref[pl.ds(at, tile), :] = total_ref[pl.ds(at, tile), :] * shrink + jnp.dot(
                    p, values, preferred_element_type=jnp.float32
                )
            return 0

        lax.fori_loop(0, (length + CHUNK - 1) // CHUNK, chunk, 0)
        live = block * BLK + lax.broadcasted_iota(jnp.int32, (BLK, HEAD_SIZE), 0) < size
        for head in range(heads):
            at = head * BLK
            result = total_ref[at : at + BLK, :HEAD_SIZE] / total_ref[at : at + BLK, HEAD_SIZE:]
            out_ref[:, head * HEAD_SIZE : (head + 1) * HEAD_SIZE] = jnp.where(
                live, result, 0.0
            ).astype(out_ref.dtype)


def attend(scalars, slot_of, steps, given, queries, draft, cache, bias, after):
    width = queries.shape[2]
    nodes = draft.shape[2]
    slots = cache.shape[2]
    blocks = nodes // BLK
    rows = width // HEAD_SIZE * BLK

    def request(s, ids, sizes, lengths, moves):
        return slot_of(s, ids, moves) // blocks, 0, 0, 0

    def rows_at(s, ids, sizes, lengths, moves):
        slot = slot_of(s, ids, moves)
        return slot // blocks, slot % blocks, 0

    grid_spec = pltpu.PrefetchScalarGridSpec(
        num_scalar_prefetch=4,
        grid=(steps,),
        in_specs=[
            pl.BlockSpec((1, BLK, width), rows_at),
            pl.BlockSpec((1, 2, nodes, HEAD_SIZE), request),
            pl.BlockSpec((1, 2, slots, HEAD_SIZE), request),
            pl.BlockSpec((1, BLK, nodes), rows_at),
            pl.BlockSpec(memory_space=pl.ANY),
        ],
        out_specs=pl.BlockSpec((BLK, width), lambda s, *_: (s, 0)),
        scratch_shapes=[
            pltpu.VMEM((rows, HEAD_SIZE), jnp.bfloat16),
            pltpu.VMEM((rows, HEAD_SIZE), jnp.float32),
            pltpu.VMEM((rows, 2 * HEAD_SIZE), jnp.float32),
        ],
    )
    return pl.pallas_call(
        functools.partial(attend_kernel, slot_of, given),
        out_shape=jax.ShapeDtypeStruct((steps * BLK, width), queries.dtype),
        grid_spec=grid_spec,
        cost_estimate=pl.CostEstimate(
            flops=steps * rows * (nodes + slots) * HEAD_SIZE * 4,
            bytes_accessed=4 * (nodes + slots) * HEAD_SIZE * 2 + steps * BLK * width * 4,
            transcendentals=steps * rows * (nodes + slots),
        ),
    )(*scalars, queries, draft, cache, bias, after)


def project_kernel(starts, splits, *refs):
    ours_ref, theirs_ref, weight_ref, sibling_ref = refs[:4]
    part_refs = refs[4 : 4 + len(starts)]
    out_refs = refs[4 + len(starts) : 4 + len(starts) + len(splits)]
    total_ref = refs[-1]
    total_ref[...] = jnp.dot(
        ours_ref[...], weight_ref[...], preferred_element_type=jnp.float32
    ) + jnp.dot(theirs_ref[...], sibling_ref[...], preferred_element_type=jnp.float32)
    for start, part_ref in zip(starts, part_refs):
        total_ref[start : start + part_ref.shape[0], :] += part_ref[...].astype(jnp.float32)
    start = 0
    for count, out_ref in zip(splits, out_refs):
        out_ref[...] = total_ref[start : start + count, :].astype(out_ref.dtype)
        start += count


def project(rows, weight, sibling, parts, splits):
    ours, theirs = rows
    count, depth = ours.shape
    columns = weight.shape[1]
    tile = math.gcd(columns, COLUMNS)

    def band(size):
        return pl.BlockSpec((size, tile), lambda s: (0, s))

    whole = pl.BlockSpec((count, depth), lambda s: (0, 0))
    return pl.pallas_call(
        functools.partial(project_kernel, tuple(start for start, _ in parts), splits),
        out_shape=[jax.ShapeDtypeStruct((size, columns), ours.dtype) for size in splits],
        grid=(columns // tile,),
        in_specs=[whole, whole, band(depth), band(depth)]
        + [band(part.shape[0]) for _, part in parts],
        out_specs=[band(size) for size in splits],
        scratch_shapes=[pltpu.VMEM((count, tile), jnp.float32)],
        cost_estimate=pl.CostEstimate(
            flops=4 * count * depth * columns,
            bytes_accessed=4 * depth * columns + 4 * count * columns,
            transcendentals=0,
        ),
        name="project",
    )(ours, theirs, weight, sibling, *(part for _, part in parts))


def local(
    queries, draft_key_value, cache_kv, out_weight, tree_sizes, parents, cache_lens, block_moves
):
    requests, nodes, width = queries.shape
    blocks = nodes // BLK
    dp_count = lax.axis_size("dp")
    mine = lax.axis_index("dp")
    tensor_count = lax.axis_size("tensor")
    spot = lax.axis_index("tensor")
    pairs = tensor_count // 2
    high, low = spot // 2, spot % 2
    ids = jnp.stack([mine, high, low]).astype(jnp.int32)
    scalars = (ids, tree_sizes, cache_lens, block_moves)
    sibling_weight = swapped(out_weight, "tensor", 1)
    bias = reach_bias(ids, parents, requests)
    per_pair = requests * blocks // pairs
    per_core = per_pair // 2

    def cores_share(rows):
        ours = lax.dynamic_index_in_dim(rows, low, 0, keepdims=False)
        theirs = lax.dynamic_index_in_dim(rows, 1 - low, 0, keepdims=False)
        return ours, swapped(theirs, "tensor", 1)

    def kept_rows(hop, first, count, giving, after):
        def slot_of(s, ids, moves):
            part = (ids[1] + hop) % pairs
            slot = part * per_pair + (s // count) * per_core + first + s % count
            return jnp.where(s >= 2 * count, moves[ids[0], 1], slot)

        rows = attend(
            scalars, slot_of, 2 * count + giving, 2 * count, queries, draft_key_value,
            cache_kv, bias, after,
        )
        split = 2 * count * BLK
        return cores_share(rows[:split].reshape(2, count * BLK, width)), rows[split:]

    def onward(part, hop):
        ring = [
            (2 * h + l, 2 * ((h + hop) % pairs) + l) for h in range(pairs) for l in range(2)
        ]
        return lax.ppermute(part, "tensor", ring)

    coming = [[] for _ in range(per_core)]
    after = bias
    for hop in range(1, pairs):
        for sub in range(per_core):
            giving = int((hop, sub) == (1, per_core - 1))
            rows, given = kept_rows(hop, sub, 1, giving, after)
            (part,) = project(rows, out_weight, sibling_weight, (), (BLK,))
            coming[sub].append(onward(part, hop))
            after = part
            if giving:
                target = block_moves[:, 0]
                numbers = jnp.arange(dp_count, dtype=jnp.int32)
                arrives = (target == mine) & (target != numbers)
                present = jnp.any(arrives)
                bits = jnp.bitwise_xor(jnp.sum(jnp.where(arrives, numbers, 0)), mine)
                arrived = jnp.zeros_like(given)
                for bit in range(dp_count.bit_length() - 1):
                    fresh = swapped(given, "dp", 1 << bit)
                    arrived = jnp.where(present & (bits == 1 << bit), fresh, arrived)
                arrived = arrived.reshape(pairs, 2, -1, width)
    ours, _ = kept_rows(0, 0, per_core, 0, after)

    def new_rows(hop):
        part = lax.dynamic_index_in_dim(arrived, (high + hop) % pairs, 0, keepdims=False)
        return cores_share(part)

    new_coming = []
    for hop in range(1, pairs):
        rows = new_rows(hop)
        (part,) = project(rows, out_weight, sibling_weight, (), (rows[0].shape[0],))
        new_coming.append(onward(part, hop))
    rows = [jnp.concatenate(two, axis=0) for two in zip(ours, new_rows(0))]
    parts = [(sub * BLK, part) for sub in range(per_core) for part in coming[sub]]
    share = per_core * BLK
    parts += [(share, part) for part in new_coming]
    return project(
        rows, out_weight, sibling_weight, parts, (share, rows[0].shape[0] - share)
    )


def solution(mesh):
    in_specs = (
        P("dp", None, "tensor"),
        P("dp", None, None, "tensor"),
        P("dp", None, None, "tensor"),
        P("tensor", None),
        P(),
        P(),
        P(),
        P(),
    )
    out_specs = (P(("dp", "tensor"), None), P(("dp", "tensor"), None))

    def build(queries, *rest):
        step = jax.shard_map(
            local, mesh=mesh, in_specs=in_specs, out_specs=out_specs, check_vma=False
        )
        return step(queries, *rest)

    return build
```
